32 devices in a mesh: rep: 4 (over x, y), dp: 8 (over z, core).
Axes of the slice: x: 2, y: 2, z: 4, core: 2. Of those that a mesh axis runs over, the one named last changes fastest.
Arguments:
- x: bfloat16 [32, 2048, 1024], P(('rep', 'dp')), parts along dimension 0
- dy: bfloat16 [32, 2048, 1024], P(('rep', 'dp')), parts along dimension 0
- w_gate: bfloat16 [2, 1024, 4096], replicated
- w_up: bfloat16 [2, 1024, 4096], replicated
- w_down: bfloat16 [2, 4096, 1024], replicated
- m_w_gate: float32 [2, 1024, 4096], P(None, 'dp')
- m_w_up: float32 [2, 1024, 4096], P(None, 'dp')
- m_w_down: float32 [2, 4096, 1024], P(None, 'dp')
- v_w_gate: float32 [2, 1024, 4096], P(None, 'dp')
- v_w_up: float32 [2, 1024, 4096], P(None, 'dp')
- v_w_down: float32 [2, 4096, 1024], P(None, 'dp')
Outputs:
- output 1: bfloat16 [8, 1024, 4096], P('rep'), parts along dimension 0
- output 2: bfloat16 [8, 1024, 4096], P('rep'), parts along dimension 0
- output 3: bfloat16 [8, 4096, 1024], P('rep'), parts along dimension 0
- output 4: float32 [8, 1024, 4096], P('rep', 'dp'), parts along dimension 0
- output 5: float32 [8, 1024, 4096], P('rep', 'dp'), parts along dimension 0
- output 6: float32 [8, 4096, 1024], P('rep', 'dp'), parts along dimension 0
- output 7: float32 [8, 1024, 4096], P('rep', 'dp'), parts along dimension 0
- output 8: float32 [8, 1024, 4096], P('rep', 'dp'), parts along dimension 0
- output 9: float32 [8, 4096, 1024], P('rep', 'dp'), parts along dimension 0
There are 4 independent parts. The reference program is written for one: setup_inputs(seed, part) draws one part's arguments, and reference() takes and returns one part's arrays. A program takes and returns all parts, laid end to end along the dimension named above; an argument that names none is the same for every part.
All inputs are finite; a program needn't handle non-finite values.
Results may differ from the reference program's by a relative error of at most 0.022.
Values are sent between devices in bfloat16 or wider.
A program may use at most 2 GiB of HBM per device.

```python
import jax
import jax.numpy as jnp
from jax import lax

SEQUENCES = 8
TOKENS = 2048
D = 1024
FF = 4096
LAYERS = 2
NAMES = ("w_gate", "w_up", "w_down")
SHAPES = {"w_gate": (LAYERS, D, FF), "w_up": (LAYERS, D, FF), "w_down": (LAYERS, FF, D)}


def bump(key, n, height):
    away = (jnp.arange(n, dtype=jnp.int32) - jax.random.randint(key, (), 0, n, jnp.int32)) % n
    return jnp.where(away < n // 8, height, 1.0)


def together(key, own, strength):
    shared = jax.random.normal(key, own.shape[1:], jnp.float32)
    return (own + strength * shared) * lax.rsqrt(1 + strength * strength)


def setup_inputs(seed: int = 0, part: int = 0) -> dict:
    kx, kdy, ka, kb, kz, kf, kh, kl, *keys = jax.random.split(jax.random.key(seed), 8 + 3 * len(NAMES))
    kx, kdy, ka, kb = (jax.random.fold_in(k, part) for k in (kx, kdy, ka, kb))
    kw, km, kv = (keys[i::3] for i in range(3))
    shape = (SEQUENCES, TOKENS, D)
    much_x, much_dy = jax.random.uniform(kz, (2,), jnp.float32, 0.0, 1.0)
    loud = 2.0 ** jax.random.uniform(jax.random.fold_in(kz, 1), (), jnp.float32, -1.0, 2.0)
    layers = 2.0 ** jax.random.uniform(kl, (LAYERS, 1, 1), jnp.float32, -1.0, 1.0)
    x = together(ka, jax.random.normal(kx, shape, jnp.float32), much_x) * bump(kf, D, 4.0)
    dy = together(kb, jax.random.normal(kdy, shape, jnp.float32), much_dy)
    drawn = {"x": x.astype(jnp.bfloat16), "dy": (loud * dy * (SEQUENCES * TOKENS) ** -0.5).astype(jnp.bfloat16)}
    for key, name in zip(kw, NAMES, strict=True):
        w = jax.random.normal(key, SHAPES[name], jnp.float32) * SHAPES[name][1] ** -0.5
        drawn[name] = (w * {"w_gate": 1.0, "w_up": bump(kh, FF, 4.0), "w_down": layers}[name]).astype(jnp.bfloat16)
    for key, name in zip(km, NAMES, strict=True):
        drawn[f"m_{name}"] = 0.1 * jax.random.normal(key, SHAPES[name], jnp.float32)
    for key, name in zip(kv, NAMES, strict=True):
        drawn[f"v_{name}"] = jax.random.uniform(key, SHAPES[name], jnp.float32, 0.005, 0.015)
    return drawn


def matmul(a, w):
    return jnp.dot(a, w, preferred_element_type=jnp.float32).astype(jnp.bfloat16)


def normed(h):
    wide = h.astype(jnp.float32)
    scale = lax.rsqrt(jnp.mean(wide**2, -1, keepdims=True) + 1e-6)
    return (wide * scale).astype(jnp.bfloat16)


def layer(h, w):
    a = normed(h)
    gate = jnp.dot(a, w["w_gate"], preferred_element_type=jnp.float32)
    up = jnp.dot(a, w["w_up"], preferred_element_type=jnp.float32)
    return h + matmul((jax.nn.silu(gate) * up).astype(jnp.bfloat16), w["w_down"])


def adamw(w, m, v, g):
    m = 0.9 * m + 0.1 * g
    v = 0.95 * v + 0.05 * g * g
    step = m * lax.rsqrt(v + 1e-8) + 0.1 * w
    return (w - 0.02 * step).astype(jnp.bfloat16), m, v


def clipped(gradients, sum_of_squares, count):
    factor = jnp.minimum(1.0, 0.5 * lax.rsqrt(sum_of_squares / count + 1e-30))
    return [g * factor for g in gradients]


def stack(weights, h):
    return lax.scan(lambda h, w: (layer(h, w), None), h, weights)[0]


def reference(x, dy, w_gate, w_up, w_down, m_w_gate, m_w_up, m_w_down, v_w_gate, v_w_up, v_w_down):
    weights = dict(zip(NAMES, (w_gate, w_up, w_down), strict=True))

    def take(so_far, sequence):
        h, by_y = sequence
        _, back = jax.vjp(lambda w: stack(w, h), weights)
        return jax.tree.map(lambda total, term: total + term.astype(jnp.float32), so_far, back(by_y)[0]), None

    none_yet = {name: jnp.zeros(w.shape, jnp.float32) for name, w in weights.items()}
    by_weights, _ = lax.scan(take, none_yet, (x, dy))
    gradients = [by_weights[name].astype(jnp.bfloat16).astype(jnp.float32) for name in NAMES]
    gradients = clipped(gradients, sum(jnp.sum(g * g) for g in gradients), sum(g.size for g in gradients))
    new = [
        adamw(w.astype(jnp.float32), m, v, g)
        for w, m, v, g in zip((w_gate, w_up, w_down), (m_w_gate, m_w_up, m_w_down), (v_w_gate, v_w_up, v_w_down), gradients, strict=True)
    ]
    return tuple(one[which] for which in range(3) for one in new)
```

```python
import jax
import jax.numpy as jnp
from jax import lax
from jax.sharding import PartitionSpec as P


F32, BF16 = jnp.float32, jnp.bfloat16
CHIPS, CORES = 4, 2
SWAP = [(i, i ^ 1) for i in range(CHIPS * CORES)]
LINES = [[chip * CORES + core for chip in range(CHIPS)] for core in range(CORES)]


def dot(a, b, contract):
    return lax.dot_general(a, b, ((contract[:1], contract[1:]), ((), ())), preferred_element_type=F32)


def normed(h):
    wide = h.astype(F32)
    scale = lax.rsqrt(jnp.mean(wide**2, -1, keepdims=True) + 1e-6)
    return (wide * scale).astype(BF16)


def adamw(w, m, v, g):
    m = 0.9 * m + 0.1 * g
    v = 0.95 * v + 0.05 * g * g
    step = m * lax.rsqrt(v + 1e-8) + 0.1 * w
    return (w - 0.02 * step).astype(BF16), m, v


def inner(h, w_gate, w_up):
    a = normed(h)
    gate, up = dot(a, w_gate, (1, 0)), dot(a, w_up, (1, 0))
    return a, gate, up, (jax.nn.silu(gate) * up).astype(BF16)


def to_inner(d_out, gate, up, w_down):
    d_hidden = dot(d_out, w_down, (1, 1)).astype(BF16).astype(F32)
    s = jax.nn.sigmoid(gate)
    silu = gate * s
    d_gate = d_hidden * up * (s + silu * (1 - s))
    return d_gate.astype(BF16), (d_hidden * silu).astype(BF16)


class Term:
    def __init__(self, core, term):
        blocks = term.astype(BF16).reshape(CHIPS, CORES, -1, term.shape[-1])
        self.own = lax.dynamic_index_in_dim(blocks, core, 1, keepdims=False)
        self.out = lax.dynamic_index_in_dim(blocks, 1 - core, 1, keepdims=False)

    def swap(self):
        other = lax.ppermute(self.out, "dp", SWAP)
        self.sums = (self.own.astype(F32) + other.astype(F32)).astype(BF16)

    def sum(self):
        sums = self.sums.reshape(-1, self.sums.shape[-1])
        return lax.psum_scatter(sums, "dp", scatter_dimension=0, tiled=True, axis_index_groups=LINES).astype(F32)


hold = lax.optimization_barrier


def body(x, dy, w_gate, w_up, w_down, *moments):
    me = lax.axis_index("dp")
    core = lax.rem(me, CORES)
    h0, dy = x[0], dy[0]
    a0, gate0, _, hidden0 = inner(h0, w_gate[0], w_up[0])
    h1 = h0 + dot(hidden0, w_down[0], (1, 0)).astype(BF16)
    a1, gate1, up1, hidden1 = inner(h1, w_gate[1], w_up[1])

    down1 = Term(core, dot(hidden1, dy, (0, 0)))
    down1.swap()
    dy, down1.sums = hold((dy, down1.sums))
    g_down1 = down1.sum()

    d_gate1, d_up1 = to_inner(dy, gate1, up1, w_down[1])
    gate_1 = Term(core, dot(a1, d_gate1, (0, 0)))
    d_up1, gate_1.out = hold((d_up1, gate_1.out))
    gate_1.swap()
    up_1 = Term(core, dot(a1, d_up1, (0, 0)))
    d_gate1, d_up1, gate_1.sums, up_1.out = hold((d_gate1, d_up1, gate_1.sums, up_1.out))
    g_gate1 = gate_1.sum()
    up_1.swap()
    d_a1 = dot(d_gate1, w_gate[1], (1, 1)).astype(BF16) + dot(d_up1, w_up[1], (1, 1)).astype(BF16)
    d_h1 = dy + jax.vjp(normed, h1)[1](d_a1)[0]
    d_h1, up_1.sums, a0_again = hold((d_h1, up_1.sums, a0))
    g_up1 = up_1.sum()

    down0 = Term(core, dot(hidden0, d_h1, (0, 0)))
    d_h1, down0.out = hold((d_h1, down0.out))
    down0.swap()
    up0 = dot(a0_again, w_up[0], (1, 0))
    d_gate0, d_up0 = to_inner(d_h1, gate0, up0, w_down[0])
    d_gate0, d_up0, down0.sums = hold((d_gate0, d_up0, down0.sums))
    g_down0 = down0.sum()
    gate_0 = Term(core, dot(a0, d_gate0, (0, 0)))
    d_up0, gate_0.out = hold((d_up0, gate_0.out))
    gate_0.swap()
    up_0 = Term(core, dot(a0, d_up0, (0, 0)))
    up_0.out, gate_0.sums = hold((up_0.out, gate_0.sums))
    g_gate0 = gate_0.sum()
    up_0.swap()
    g_up0 = up_0.sum()

    gradients = [(g_gate0, g_gate1), (g_up0, g_up1), (g_down0, g_down1)]
    squares = sum(jnp.sum(g * g) for pair in gradients for g in pair)
    for distance in (1, 2, 4):
        squares = squares + lax.ppermute(squares, "dp", [(i, i ^ distance) for i in range(CHIPS * CORES)])
    count = w_gate.size + w_up.size + w_down.size
    factor = jnp.minimum(1.0, 0.5 * lax.rsqrt(squares / count + 1e-30))
    new = []
    for w, m, v, pair in zip((w_gate, w_up, w_down), moments[:3], moments[3:], gradients, strict=True):
        own = lax.dynamic_slice_in_dim(w, me * m.shape[1], m.shape[1], 1).astype(F32)
        new.append(adamw(own, m, v, jnp.stack(pair) * factor))
    (own_gate, own_up, own_down), new_m, new_v = zip(*new)
    blocks_down, blocks_gate = (lax.all_gather(own, "dp") for own in (own_down, own_gate))
    new_down = laid_out(blocks_down)
    own_up, new_down = hold((own_up, new_down))
    blocks_up, new_gate = hold((lax.all_gather(own_up, "dp"), laid_out(blocks_gate)))
    return new_gate, laid_out(blocks_up), new_down, *new_m, *new_v


def laid_out(blocks):
    return blocks.transpose(1, 0, 2, 3).reshape(blocks.shape[1], -1, blocks.shape[3])


def solution(mesh):
    data, whole, rows = P(("rep", "dp")), P(), P(None, "dp")
    return jax.shard_map(
        body,
        mesh=mesh,
        in_specs=(data, data, *[whole] * 3, *[rows] * 6),
        out_specs=(*[P("rep")] * 3, *[P("rep", "dp")] * 6),
        check_vma=False,
    )
```

```python
import jax
import jax.numpy as jnp
from jax import lax
from jax.sharding import PartitionSpec as P


F32, BF16 = jnp.float32, jnp.bfloat16
CHIPS, CORES = 4, 2
SWAP = [(i, i ^ 1) for i in range(CHIPS * CORES)]
LINES = [[chip * CORES + core for chip in range(CHIPS)] for core in range(CORES)]


def dot(a, b, contract):
    return lax.dot_general(a, b, ((contract[:1], contract[1:]), ((), ())), preferred_element_type=F32)


def normed(h):
    wide = h.astype(F32)
    scale = lax.rsqrt(jnp.mean(wide**2, -1, keepdims=True) + 1e-6)
    return (wide * scale).astype(BF16)


def adamw(w, m, v, g):
    m = 0.9 * m + 0.1 * g
    v = 0.95 * v + 0.05 * g * g
    step = m * lax.rsqrt(v + 1e-8) + 0.1 * w
    return (w - 0.02 * step).astype(BF16), m, v


def inner(h, w_gate, w_up):
    a = normed(h)
    gate, up = dot(a, w_gate, (1, 0)), dot(a, w_up, (1, 0))
    return a, gate, up, (jax.nn.silu(gate) * up).astype(BF16)


def to_inner(d_out, gate, up, w_down):
    d_hidden = dot(d_out, w_down, (1, 1)).astype(BF16).astype(F32)
    s = jax.nn.sigmoid(gate)
    silu = gate * s
    d_gate = d_hidden * up * (s + silu * (1 - s))
    return d_gate.astype(BF16), (d_hidden * silu).astype(BF16)


class Term:
    def __init__(self, core, term):
        blocks = term.astype(BF16).reshape(CHIPS, CORES, -1, term.shape[-1])
        self.own = lax.dynamic_index_in_dim(blocks, core, 1, keepdims=False)
        self.out = lax.dynamic_index_in_dim(blocks, 1 - core, 1, keepdims=False)

    def swap(self):
        other = lax.ppermute(self.out, "dp", SWAP)
        self.sums = (self.own.astype(F32) + other.astype(F32)).astype(BF16)

    def sum(self):
        sums = self.sums.reshape(-1, self.sums.shape[-1])
        return lax.psum_scatter(sums, "dp", scatter_dimension=0, tiled=True, axis_index_groups=LINES).astype(F32)


hold = lax.optimization_barrier


def body(x, dy, w_gate, w_up, w_down, *moments):
    me = lax.axis_index("dp")
    core = lax.rem(me, CORES)
    h0, dy = x[0], dy[0]
    a0, gate0, up0, hidden0 = inner(h0, w_gate[0], w_up[0])
    h1 = h0 + dot(hidden0, w_down[0], (1, 0)).astype(BF16)
    a1, gate1, up1, hidden1 = inner(h1, w_gate[1], w_up[1])

    down1 = Term(core, dot(hidden1, dy, (0, 0)))
    down1.swap()
    dy, down1.sums = hold((dy, down1.sums))
    g_down1 = down1.sum()

    d_gate1, d_up1 = to_inner(dy, gate1, up1, w_down[1])
    gate_1 = Term(core, dot(a1, d_gate1, (0, 0)))
    gate_1.swap()
    d_up1, gate_1.sums = hold((d_up1, gate_1.sums))
    up_1 = Term(core, dot(a1, d_up1, (0, 0)))
    d_gate1, d_up1, up_1.out = hold((d_gate1, d_up1, up_1.out))
    g_gate1 = gate_1.sum()
    up_1.swap()
    d_a1 = dot(d_gate1, w_gate[1], (1, 1)).astype(BF16) + dot(d_up1, w_up[1], (1, 1)).astype(BF16)
    d_h1 = dy + jax.vjp(normed, h1)[1](d_a1)[0]
    d_h1, up_1.sums = hold((d_h1, up_1.sums))
    g_up1 = up_1.sum()

    down0 = Term(core, dot(hidden0, d_h1, (0, 0)))
    d_h1, down0.out = hold((d_h1, down0.out))
    down0.swap()
    d_gate0, d_up0 = to_inner(d_h1, gate0, up0, w_down[0])
    d_gate0, d_up0, down0.sums = hold((d_gate0, d_up0, down0.sums))
    g_down0 = down0.sum()
    gate_0 = Term(core, dot(a0, d_gate0, (0, 0)))
    d_up0, gate_0.out = hold((d_up0, gate_0.out))
    gate_0.swap()
    up_0 = Term(core, dot(a0, d_up0, (0, 0)))
    up_0.out, gate_0.sums = hold((up_0.out, gate_0.sums))
    g_gate0 = gate_0.sum()
    up_0.swap()
    g_up0 = up_0.sum()

    gradients = [(g_gate0, g_gate1), (g_up0, g_up1), (g_down0, g_down1)]
    squares = sum(jnp.sum(g * g) for pair in gradients for g in pair)
    for distance in (1, 2, 4):
        squares = squares + lax.ppermute(squares, "dp", [(i, i ^ distance) for i in range(CHIPS * CORES)])
    count = w_gate.size + w_up.size + w_down.size
    factor = jnp.minimum(1.0, 0.5 * lax.rsqrt(squares / count + 1e-30))
    new = []
    for w, m, v, pair in zip((w_gate, w_up, w_down), moments[:3], moments[3:], gradients, strict=True):
        own = lax.dynamic_slice_in_dim(w, me * m.shape[1], m.shape[1], 1).astype(F32)
        new.append(adamw(own, m, v, jnp.stack(pair) * factor))
    (own_gate, own_up, own_down), new_m, new_v = zip(*new)
    blocks_down, blocks_gate = (lax.all_gather(own, "dp") for own in (own_down, own_gate))
    new_down = laid_out(blocks_down)
    own_up, new_down = hold((own_up, new_down))
    blocks_up, new_gate = hold((lax.all_gather(own_up, "dp"), laid_out(blocks_gate)))
    return new_gate, laid_out(blocks_up), new_down, *new_m, *new_v


def laid_out(blocks):
    return blocks.transpose(1, 0, 2, 3).reshape(blocks.shape[1], -1, blocks.shape[3])


def solution(mesh):
    data, whole, rows = P(("rep", "dp")), P(), P(None, "dp")
    return jax.shard_map(
        body,
        mesh=mesh,
        in_specs=(data, data, *[whole] * 3, *[rows] * 6),
        out_specs=(*[P("rep")] * 3, *[P("rep", "dp")] * 6),
        check_vma=False,
    )
```
